32 devices in a mesh: grp: 1, dev: 32 (over z, y, x, core).
Axes of the slice: x: 2, y: 2, z: 4, core: 2. Of those that a mesh axis runs over, the one named last changes fastest.
Arguments:
- points: float32 [32768, 768], P(('grp', 'dev')), may hold values from -12 to 12
- assignment: int32 [32768], P(('grp', 'dev')), may hold values from 0 to 8191, as said below
Outputs:
- centroids: float32 [8192, 768], P('dev')
- spread: float32 [8192], P('dev')
The draws below stay inside these ranges and needn't reach their ends.
Inputs may be any that keep to these rules, and one draw needn't show every extreme that they name: `assignment`: the owner of cluster c is c // 256. Among the 1024 points of one device (aligned blocks of 1024), at most 64 belong to clusters of one owner; some owner receives exactly 64 from every device's block.
All inputs are finite; a program needn't handle non-finite values.
Results may differ from the reference program's by a relative error of at most 0.000071.
Values sent between devices are 32-bit elements; how exact they have to be, the bound alone decides.
A program may use at most 64 MiB of HBM per device.

```python
import jax
import jax.numpy as jnp
from jax import lax

D = 768
CL_OWN = 256
TOK_DEV = 1024
CLUSTERS = 8192
CAP = 64
POINTS = 32768


def draw_assignment(key, part):
    blocks = POINTS // TOK_DEV
    owners = CLUSTERS // CL_OWN
    total_slots = owners * CAP
    key_hot, key_score, key_order, key_within = jax.random.split(key, 4)
    hottest = jax.random.randint(key_hot, (), 0, owners)
    scores = jax.random.randint(key_score, (blocks, total_slots), 0, 1 << 16)
    slot_owner = jnp.arange(total_slots, dtype=jnp.int32) // CAP
    scores = jnp.where(slot_owner[None, :] == hottest, scores + (1 << 17), scores)
    distinct = scores * total_slots + jnp.arange(total_slots, dtype=jnp.int32)[None, :]
    _, chosen = lax.top_k(distinct, TOK_DEV)
    shuffle = jax.random.randint(key_order, (blocks, TOK_DEV), 0, 1 << 18)
    shuffle = shuffle * TOK_DEV + jnp.arange(TOK_DEV, dtype=jnp.int32)[None, :]
    order = jnp.argsort(shuffle, axis=1)
    picked = jnp.take_along_axis(chosen.astype(jnp.int32), order, axis=1)
    owner = picked // CAP
    within = jax.random.randint(key_within, (blocks, TOK_DEV), 0, CL_OWN)
    return (owner * CL_OWN + within).reshape(-1).astype(jnp.int32)


def block_levels(stream_key, dims, shards, smallest, largest):
    gain, own = 1.0, jax.random.fold_in(stream_key, 6)
    for dim, parts in shards:
        steps = jnp.exp(jax.random.uniform(jax.random.fold_in(own, dim), (parts,), jnp.float32, smallest / len(shards), largest / len(shards)))
        gain = gain * jnp.repeat(steps, dims[dim] // parts).reshape([-1 if axis == dim else 1 for axis in range(len(dims))])
    return gain


def bell_draw(stream_key, extent, width, limit, shards=(), held_as=jnp.bfloat16):
    drawn = width * jax.random.normal(stream_key, extent, jnp.float32)
    if shards:
        drawn = drawn * block_levels(stream_key, extent, shards, -0.22, 0.18)
    return jnp.clip(drawn, -limit, limit).astype(held_as)


def setup_inputs(seed: int = 0) -> dict:
    key_of = jax.random.split(jax.random.key(seed), 3)
    points = bell_draw(key_of[0], (POINTS, D), 2.0, 12.0, ((0, 32),), jnp.float32)
    assignment = draw_assignment(jax.random.fold_in(key_of[2], 71), 0)
    return dict(points=points, assignment=assignment)


def reference(points, assignment):
    sums = jax.ops.segment_sum(points, assignment, num_segments=CLUSTERS)
    counts = jax.ops.segment_sum(jnp.ones(assignment.shape, jnp.float32), assignment, num_segments=CLUSTERS)
    squares = jax.ops.segment_sum(jnp.sum(points * points, axis=1), assignment, num_segments=CLUSTERS)
    denom = jnp.maximum(counts, 1.0)
    centroids = sums / denom[:, None]
    spread = (squares - jnp.sum(sums * sums, axis=1) / denom) / (denom * D)
    return centroids, spread
```

```python
import functools

import jax
import jax.numpy as jnp
from jax import lax
from jax.experimental import pallas as pl
from jax.experimental.pallas import tpu as pltpu
from jax.sharding import PartitionSpec as P

CL_OWN = 256
LANES = 128
INNER = 8
MESH = pl.DeviceIdType.MESH


def finish(sums, counts, squares):
    denom = jnp.maximum(counts, 1.0)
    centre = sums / denom[:, None]
    spread = (squares - jnp.sum(sums * sums, axis=1) / denom) / (denom * sums.shape[1])
    return (centre, spread)


def pieces(value, count):
    out = []
    for _ in range(count):
        part = value.astype(jnp.bfloat16)
        out.append(part)
        value = value - part.astype(jnp.float32)
    return out


def kernel(
    outer, cap, chunk, alone,
    points_ref, label_ref, main_ref, side_ref,
    stage, high, low, norm, facts, hit, hold, cout, xin, yin, mout, mgot, zout, zin, zaux, zin_aux,
    total, aux_all,
    lsem, msend, mrecv, csend, crecv, fsend, frecv, dsend, drecv, psend, precv,
    zsend, zrecv, asend, arecv, osem,
):
    inner = INNER
    me = lax.axis_index("dev")
    plane = me // inner
    seat = lax.rem(me, inner)
    rows, width = points_ref.shape
    owners = inner * outer
    chunks = width // chunk
    wide = chunk // 2
    rep = LANES // cap
    last = outer - 1
    rights, lefts = last - plane, plane
    steps = outer * chunks
    half = inner // 2 * cap
    ring = cout.shape[0]

    core = lax.rem(seat, 2)
    x = lax.rem(seat // 2, 2)
    y = seat // 4

    def target_plane(j):
        if j == last:
            return plane
        right_first = jnp.where(j < rights, last - j, j - rights)
        left_first = jnp.where(j < lefts, j, last - j + lefts)
        return jnp.where(rights > lefts, right_first, left_first)

    def fed(j):
        k = target_plane(j)
        return jnp.where(k > plane, plane > 0, plane < last)

    def across(d):
        other = 0
        for bit in range(3):
            own = lax.rem(seat // 2**bit, 2)
            other = other + (1 - own if d // 2**bit % 2 else own) * 2**bit
        return other

    def load(c):
        return pltpu.make_async_copy(
            points_ref.at[:, pl.ds(c * chunk, chunk)], stage.at[c], lsem.at[c]
        )

    def plane_copy(src, dst, ssem, rsem, d):
        return pltpu.make_async_remote_copy(
            src_ref=src,
            dst_ref=dst,
            send_sem=ssem,
            recv_sem=rsem,
            device_id={"dev": plane * inner + across(d)},
            device_id_type=MESH,
        )

    def core_copy(t):
        return plane_copy(
            cout.at[t % ring], hold.at[t, :, :, :, core], csend.at[t], crecv.at[t], 1
        )

    def core_arrival(t):
        return plane_copy(
            cout.at[t % ring], hold.at[t, :, :, :, 1 - core], csend.at[t], crecv.at[t], 1
        )

    def parts_of(t):
        return 2 if t == 0 else 1

    def first_copy(t, h, part):
        source = hold.at[t, 0, 1 - x] if h == 0 else hold.at[t, 1, :, 1 - y]
        target = xin.at[t, h]
        if parts_of(t) == 2:
            of = core if part == 0 else 1 - core
            source = hold.at[t, 0, 1 - x, :, of] if h == 0 else hold.at[t, 1, :, 1 - y, of]
            target = xin.at[t, h, :, of]
        return plane_copy(source, target, fsend.at[t, h, part], frecv.at[t, h, part], 2 if h == 0 else 4)

    def direct_copy(t, h):
        source = hold.at[t, 0, x, 1 - y] if h == 0 else hold.at[t, 1, 1 - x, y]
        return plane_copy(source, yin.at[t, h, 0], dsend.at[t, h], drecv.at[t, h], 4 if h == 0 else 2)

    def passed_copy(t, h):
        source = xin.at[t, 0, 1 - y] if h == 0 else xin.at[t, 1, 1 - x]
        return plane_copy(source, yin.at[t, h, 1], psend.at[t, h], precv.at[t, h], 4 if h == 0 else 2)

    def meta_copy(d, arriving):
        return plane_copy(
            mout.at[across(d)], mgot.at[across(d) if arriving else seat],
            msend.at[d], mrecv.at[d], d,
        )

    def line_copy(j, c):
        k = target_plane(j)
        step = jnp.where(k > plane, 1, -1)
        place = jnp.where(k == plane - 1, outer, k)
        return pltpu.make_async_remote_copy(
            src_ref=zout.at[j, c],
            dst_ref=zin.at[place, c],
            send_sem=zsend.at[j, c],
            recv_sem=zrecv.at[place, c],
            device_id={"dev": (plane + step) * inner + seat},
            device_id_type=MESH,
        )

    def line_arrival(place, c):
        side = jnp.where(plane > 0, -1, 1)
        return pltpu.make_async_remote_copy(
            src_ref=zout.at[0, c],
            dst_ref=zin.at[place, c],
            send_sem=zsend.at[0, c],
            recv_sem=zrecv.at[place, c],
            device_id={"dev": (plane + side) * inner + seat},
            device_id_type=MESH,
        )

    def aux_copy(j, arriving):
        k = target_plane(j)
        return pltpu.make_async_remote_copy(
            src_ref=zaux.at[j],
            dst_ref=zin_aux.at[k if arriving else plane],
            send_sem=asend.at[j],
            recv_sem=arecv.at[k if arriving else plane],
            device_id={"dev": k * inner + seat},
            device_id_type=MESH,
        )

    def route():
        label = label_ref[...]
        owner = lax.shift_right_logical(label, CL_OWN.bit_length() - 1)
        row = lax.broadcasted_iota(jnp.int32, (LANES, 2 * LANES), 0)
        col = lax.broadcasted_iota(jnp.int32, (LANES, 2 * LANES), 1)
        before = jnp.logical_or(row < col, col >= LANES).astype(jnp.bfloat16)
        index = lax.broadcasted_iota(jnp.int32, (owners, LANES), 0)
        blocks = rows // LANES
        marks = [
            (index == owner[:, b * LANES : (b + 1) * LANES]).astype(jnp.float32)
            for b in range(blocks)
        ]
        counts = jnp.dot(
            jnp.concatenate(marks, axis=0).astype(jnp.bfloat16), before,
            preferred_element_type=jnp.float32,
        )
        running = jnp.zeros((owners, LANES), jnp.float32)
        position = []
        for b in range(blocks):
            block = counts[b * owners : (b + 1) * owners]
            place = marks[b] * (block[:, :LANES] + running)
            position.append(jnp.sum(place, axis=0, keepdims=True))
            running = running + block[:, LANES:]
        position = jnp.concatenate(position, axis=1).astype(jnp.int32)
        inside = owner & (inner - 1)
        swapped = (inside & 1) * 4 + (lax.shift_right_logical(inside, 1) & 1) * 2
        swapped = swapped + lax.shift_right_logical(inside, 2)
        return (owner - inside + swapped) * cap + position

    def picks(j, target):
        row = lax.broadcasted_iota(jnp.int32, (2 * half, 1), 0)
        slot = target_plane(j) * (2 * half) + row
        slot = slot + jnp.where(row < half, core * half, -core * half)
        return (slot == target).astype(jnp.bfloat16)

    def split(c):
        load(c).wait()
        value = stage[c]
        top = value.astype(jnp.bfloat16)
        columns = slice(c * chunk, (c + 1) * chunk)
        high[:, columns] = top
        low[:, columns] = (value - top.astype(jnp.float32)).astype(jnp.bfloat16)
        square = value * value
        square = square[:, :wide] + square[:, wide:]
        if c == 0:
            norm[...] = square
        else:
            norm[...] += square

    def gather(t, pick):
        c = t % chunks
        columns = slice(c * chunk, (c + 1) * chunk)
        if t >= ring:
            core_copy(t - ring).wait_send()
        block = jnp.dot(pick, high[:, columns], preferred_element_type=jnp.float32)
        block = block + jnp.dot(pick, low[:, columns], preferred_element_type=jnp.float32)
        for h in range(2):
            part = block[:, h * wide : (h + 1) * wide]
            hold[t, h, :, :, core] = part[:half].reshape(2, 2, cap, wide)
            cout[t % ring, h] = part[half:].reshape(2, 2, cap, wide)

    def tell():
        norms = jnp.sum(norm[...].T, axis=0, keepdims=True)
        label = (label_ref[...] & (CL_OWN - 1)) + 1
        label = label.astype(jnp.float32).astype(jnp.bfloat16)
        blank = jnp.zeros((4, rows), jnp.bfloat16)
        facts[...] = jnp.concatenate([label] + pieces(norms, 3) + [blank], axis=0)

    def tell_slots(j, pick):
        told = lax.dot_general(
            facts[...], pick, (((1,), (1,)), ((), ())), preferred_element_type=jnp.float32
        )
        told = jnp.concatenate([told[0:1], told[1:2] + told[2:3] + told[3:4]], axis=0)
        for q in range(inner):
            p = q % 2 * 4 + q // 2 % 2 * 2 + (core if q < inner // 2 else 1 - core)
            mine = told[:, q * cap : (q + 1) * cap]
            mout[p, 2 * j : 2 * j + 2] = jnp.concatenate([mine] * rep, axis=1)

    lane = lax.broadcasted_iota(jnp.int32, (8, LANES), 1)
    line = lax.broadcasted_iota(jnp.int32, (8, LANES), 0)
    cluster = lax.broadcasted_iota(jnp.int32, (CL_OWN, LANES), 0).astype(jnp.float32) + 1.0

    def matches(j):
        if j == 0:
            for d in range(1, inner):
                meta_copy(d, True).wait_recv()
            mgot[seat] = mout[seat]
        weights = []
        for s in range(inner):
            block = mgot[across(s // 2 * 2) - core + s % 2, 2 * j : 2 * j + 2]
            hit[:, s * LANES : (s + 1) * LANES] = (cluster == block[0:1, :]).astype(jnp.bfloat16)
            weight = jnp.where(line == 0, 1.0, 0.0)
            for n, piece in enumerate(pieces(block[1:2, :], 3)):
                weight = jnp.where(line == n + 1, piece.astype(jnp.float32), weight)
            weights.append(jnp.where(lane < cap, weight, 0.0).astype(jnp.bfloat16))
        aux = lax.dot_general(
            jnp.concatenate(weights, axis=1), hit[...], (((1,), (1,)), ((), ())),
            preferred_element_type=jnp.float32,
        )
        if j < last:
            zaux[j] = aux
            aux_copy(j, False).start()
        else:
            aux_all[...] = aux

    def sources(t, h):
        own = hold.at[t, h, x, y]
        first = xin.at[t, h, y if h == 0 else x]
        direct, passed = yin.at[t, h, 0], yin.at[t, h, 1]
        return (own, first, direct, passed) if h == 0 else (own, direct, first, passed)

    def product(t, h, begin, end):
        stack = []
        for ref in sources(t, h)[begin:end]:
            for s in range(2):
                stack.extend(pieces(ref[s], rep))
        return jnp.dot(
            hit[:, begin * 2 * LANES : end * 2 * LANES], jnp.concatenate(stack, axis=0),
            preferred_element_type=jnp.float32,
        )

    def reduce(j, c):
        t = j * chunks + c
        for h in range(2):
            direct_copy(t, h).wait_recv()
        early = [product(t, h, 0, 3) for h in range(2)] if t == steps - 1 else None
        for h in range(2):
            passed_copy(t, h).wait_recv()
        for h in range(2):
            if early is None:
                value = product(t, h, 0, 4)
            else:
                value = early[h] + product(t, h, 3, 4)
            columns = slice(h * wide, (h + 1) * wide)
            if j < last:
                zout[j, c, :, columns] = value
            else:
                total[c, :, columns] = value

    def forward(j, c):
        @pl.when(fed(j))
        def _():
            line_arrival(target_plane(j), c).wait_recv()
            zout[j, c] += zin[target_plane(j), c]
            line_copy(j, c).start()

    def collect():
        for j in range(last):
            aux_copy(j, True).wait_recv()
            aux_all[...] += zin_aux[target_plane(j)]

    def settle(c):
        @pl.when(plane > 0)
        def _():
            line_arrival(plane, c).wait_recv()
            total[c] += zin[plane, c]

        @pl.when(plane < last)
        def _():
            line_arrival(outer, c).wait_recv()
            total[c] += zin[outer, c]

    def out_copy(c):
        return pltpu.make_async_copy(
            total.at[c], main_ref.at[:, pl.ds(c * chunk, chunk)], osem.at[c]
        )

    for d in range(chunks):
        load(d).start()
    barrier = pltpu.get_barrier_semaphore()
    for d in range(1, inner):
        peer = plane * inner + across(d)
        pl.semaphore_signal(barrier, inc=1, device_id={"dev": peer}, device_id_type=MESH)
    for d in range(1, outer):
        peer = lax.rem(plane + d, outer) * inner + seat
        pl.semaphore_signal(barrier, inc=1, device_id={"dev": peer}, device_id_type=MESH)

    target = route()
    pick = picks(0, target)
    split(0)
    gather(0, pick)
    pl.semaphore_wait(barrier, inner + outer - 2)
    for h in range(2):
        first_copy(0, h, 0).start()
    core_copy(0).start()
    ready = 1

    def prepare(pick):
        nonlocal ready
        t = ready
        if t < steps:
            if t < chunks:
                split(t)
            if t % chunks == 0:
                pick = picks(t // chunks, target)
            gather(t, pick)
            core_copy(t).start()
            ready += 1
        return pick

    pick = prepare(pick)
    core_arrival(0).wait_recv()
    for h in range(2):
        first_copy(0, h, 1).start()
    for h in range(2):
        direct_copy(0, h).start()
    pick = prepare(pick)
    core_arrival(1).wait_recv()
    for h in range(2):
        first_copy(1, h, 0).start()
    while ready < chunks:
        pick = prepare(pick)
    tell()
    for j in range(outer):
        tell_slots(j, picks(j, target))
    for d in range(1, inner):
        meta_copy(d, False).start()

    waiting = []

    def arrange(t):
        j, c = t // chunks, t % chunks
        if c == 0:
            matches(j)
        reduce(j, c)
        if j < last:
            @pl.when(jnp.logical_not(fed(j)))
            def _():
                line_copy(j, c).start()

            if j == last - 1:
                forward(j, c)
            else:
                waiting.append((j, c))
        while waiting and (len(waiting) > 2 or t >= last * chunks - 1):
            forward(*waiting.pop(0))

    for t in range(steps):
        for h in range(2):
            for part in range(parts_of(t)):
                first_copy(t, h, part).wait_recv()
            passed_copy(t, h).start()
        if t + 2 < steps:
            core_arrival(t + 2).wait_recv()
            for h in range(2):
                first_copy(t + 2, h, 0).start()
        if t + 1 < steps:
            for h in range(2):
                direct_copy(t + 1, h).start()
        pick = prepare(pick)
        if t > 0:
            arrange(t - 1)

    collect()
    for c in range(chunks):
        if c == chunks - 1:
            arrange(steps - 1)
        settle(c)
        if not alone:
            out_copy(c).start()
    if alone:
        counts = jnp.maximum(aux_all[0:1, :], 1.0)
        denom = jnp.broadcast_to(counts, (LANES, CL_OWN)).T
        gathered = jnp.zeros((CL_OWN, LANES), jnp.float32)
        for c in range(chunks):
            for n in range(chunk // LANES):
                columns = slice(n * LANES, (n + 1) * LANES)
                value = total[c, :, columns]
                gathered = gathered + value * value
                total[c, :, columns] = value / denom
            out_copy(c).start()
        lengths = jnp.sum(gathered.T, axis=0, keepdims=True)
        squares = aux_all[1:2, :] + aux_all[2:3, :] + aux_all[3:4, :]
        side_ref[...] = (squares - lengths / counts) / (counts * width)
    else:
        side_ref[...] = aux_all[...]

    for d in range(1, inner):
        meta_copy(d, False).wait_send()
    for t in range(steps):
        if t >= steps - ring:
            core_copy(t).wait_send()
        for h in range(2):
            for part in range(parts_of(t)):
                first_copy(t, h, part).wait_send()
            direct_copy(t, h).wait_send()
            passed_copy(t, h).wait_send()
    for j in range(last):
        aux_copy(j, False).wait_send()
        for c in range(chunks):
            line_copy(j, c).wait_send()
    for c in range(chunks):
        out_copy(c).wait()


def body(points, assignment):
    owners = lax.axis_size("dev")
    alone = lax.axis_size("grp") == 1
    rows, width = points.shape
    cap = 2 * rows // owners
    outer = owners // INNER
    chunk = 2 * LANES
    chunks = width // chunk
    wide = chunk // 2
    steps = outer * chunks
    ring = min(steps, 4)

    f32, b16 = jnp.float32, jnp.bfloat16
    dma = pltpu.SemaphoreType.DMA
    hops = max(outer - 1, 1)
    side = (1, CL_OWN) if alone else (8, CL_OWN)
    vmem = pl.BlockSpec(memory_space=pltpu.VMEM)
    hbm = pl.BlockSpec(memory_space=pltpu.HBM)
    main, side = pl.pallas_call(
        functools.partial(kernel, outer, cap, chunk, alone),
        out_shape=(
            jax.ShapeDtypeStruct((CL_OWN, width), f32),
            jax.ShapeDtypeStruct(side, f32),
        ),
        in_specs=[hbm, vmem],
        out_specs=[hbm, vmem],
        scratch_shapes=[
            pltpu.VMEM((chunks, rows, chunk), f32),
            pltpu.VMEM((rows, width), b16),
            pltpu.VMEM((rows, width), b16),
            pltpu.VMEM((rows, LANES), f32),
            pltpu.VMEM((8, rows), b16),
            pltpu.VMEM((CL_OWN, INNER * LANES), b16),
            pltpu.VMEM((steps, 2, 2, 2, 2, cap, wide), f32),
            pltpu.VMEM((ring, 2, 2, 2, cap, wide), f32),
            pltpu.VMEM((steps, 2, 2, 2, cap, wide), f32),
            pltpu.VMEM((steps, 2, 2, 2, cap, wide), f32),
            pltpu.VMEM((INNER, 2 * outer, LANES), f32),
            pltpu.VMEM((INNER, 2 * outer, LANES), f32),
            pltpu.VMEM((hops, chunks, CL_OWN, chunk), f32),
            pltpu.VMEM((outer + 1, chunks, CL_OWN, chunk), f32),
            pltpu.VMEM((hops, 8, CL_OWN), f32),
            pltpu.VMEM((outer, 8, CL_OWN), f32),
            pltpu.VMEM((chunks, CL_OWN, chunk), f32),
            pltpu.VMEM((8, CL_OWN), f32),
            dma((chunks,)),
            dma((INNER,)), dma((INNER,)),
            dma((steps,)), dma((steps,)),
            dma((steps, 2, 2)), dma((steps, 2, 2)),
            dma((steps, 2)), dma((steps, 2)),
            dma((steps, 2)), dma((steps, 2)),
            dma((hops, chunks)), dma((outer + 1, chunks)),
            dma((hops,)), dma((outer,)),
            dma((chunks,)),
        ],
        compiler_params=pltpu.CompilerParams(
            collective_id=0, has_side_effects=True, vmem_limit_bytes=63 * 1024 * 1024
        ),
    )(points, assignment.reshape(1, rows))
    if alone:
        return main, side[0]
    squares = side[1] + side[2] + side[3]
    sums, counts, squares = lax.psum((main, side[0], squares), "grp")
    return finish(sums, counts, squares)


def solution(mesh):
    return jax.shard_map(
        body,
        mesh=mesh,
        in_specs=(P(("grp", "dev"), None), P(("grp", "dev"))),
        out_specs=(P("dev", None), P("dev")),
        check_vma=False,
    )
```

```python
import functools

import jax
import jax.numpy as jnp
from jax import lax
from jax.experimental import pallas as pl
from jax.experimental.pallas import tpu as pltpu
from jax.sharding import PartitionSpec as P

CL_OWN = 256
LANES = 128
INNER = 8
LIMIT = 52 * 1024 * 1024
MESH = pl.DeviceIdType.MESH


def finish(sums, counts, squares):
    denom = jnp.maximum(counts, 1.0)
    centre = sums / denom[:, None]
    spread = (squares - jnp.sum(sums * sums, axis=1) / denom) / (denom * sums.shape[1])
    return (centre, spread)


def pieces(value, count):
    out = []
    for _ in range(count):
        part = value.astype(jnp.bfloat16)
        out.append(part)
        value = value - part.astype(jnp.float32)
    return out


def kernel(
    outer, cap, chunk, alone,
    points_ref, label_hbm, main_ref, side_ref,
    label_ref, stage, high, low, norm, facts, hit, hold, cout, xin, yin, mout, mgot, zout, zin, zaux, zin_aux,
    total, aux_all, inverse, lengths,
    lsem, msend, mrecv, csend, crecv, fsend, frecv, ysend, yrecv,
    zsend, zrecv, asend, arecv,
):
    inner = INNER
    me = lax.axis_index("dev")
    plane = me // inner
    seat = lax.rem(me, inner)
    rows, width = points_ref.shape
    owners = inner * outer
    chunks = width // chunk
    wide = chunk // 2
    rep = LANES // cap
    last = outer - 1
    rights, lefts = last - plane, plane
    steps = outer * chunks
    half = inner // 2 * cap
    ring = cout.shape[0]

    core = lax.rem(seat, 2)
    x = lax.rem(seat // 2, 2)
    y = seat // 4

    def target_plane(j):
        if j == last:
            return plane
        right_first = jnp.where(j < rights, last - j, j - rights)
        left_first = jnp.where(j < lefts, j, last - j + lefts)
        return jnp.where(rights > lefts, right_first, left_first)

    def fed(j):
        k = target_plane(j)
        return jnp.where(k > plane, plane > 0, plane < last)

    def across(d):
        other = 0
        for bit in range(3):
            own = lax.rem(seat // 2**bit, 2)
            other = other + (1 - own if d // 2**bit % 2 else own) * 2**bit
        return other

    def load_label():
        return pltpu.make_async_copy(label_hbm, label_ref, lsem.at[chunks])

    def load(c):
        return pltpu.make_async_copy(
            points_ref.at[:, pl.ds(c * chunk, chunk)], stage.at[c], lsem.at[c]
        )

    def drain(ref, sem):
        pltpu.make_async_copy(ref, ref, sem).wait()

    def plane_copy(src, dst, ssem, rsem, d):
        return pltpu.make_async_remote_copy(
            src_ref=src,
            dst_ref=dst,
            send_sem=ssem,
            recv_sem=rsem,
            device_id={"dev": plane * inner + across(d)},
            device_id_type=MESH,
        )

    def core_copy(t):
        return plane_copy(
            cout.at[t % ring], hold.at[t, :, :, :, core], csend.at[t % ring], crecv.at[t], 1
        )

    def core_arrival(t):
        return plane_copy(
            cout.at[t % ring], hold.at[t, :, :, :, 1 - core], csend.at[t % ring], crecv.at[t], 1
        )

    def parts_of(t):
        return 2 if t < 2 else 1

    def first_copy(t, h, part):
        source = hold.at[t, 0, 1 - x] if h == 0 else hold.at[t, 1, :, 1 - y]
        target = xin.at[t, h]
        if parts_of(t) == 2:
            of = core if part == 0 else 1 - core
            source = hold.at[t, 0, 1 - x, :, of] if h == 0 else hold.at[t, 1, :, 1 - y, of]
            target = xin.at[t, h, :, of]
        return plane_copy(source, target, fsend, frecv.at[t], 2 if h == 0 else 4)

    def direct_copy(t, h):
        source = hold.at[t, 0, x, 1 - y] if h == 0 else hold.at[t, 1, 1 - x, y]
        arrived = yrecv.at[steps if t == steps - 1 else t]
        return plane_copy(source, yin.at[t, h, 0], ysend, arrived, 4 if h == 0 else 2)

    def passed_copy(t, h):
        source = xin.at[t, 0, 1 - y] if h == 0 else xin.at[t, 1, 1 - x]
        return plane_copy(source, yin.at[t, h, 1], ysend, yrecv.at[t], 4 if h == 0 else 2)

    def meta_copy(d):
        return plane_copy(mout.at[across(d)], mgot.at[seat], msend, mrecv, d)

    def line_copy(j, c):
        k = target_plane(j)
        step = jnp.where(k > plane, 1, -1)
        place = jnp.where(k == plane - 1, outer, k)
        return pltpu.make_async_remote_copy(
            src_ref=zout.at[j, c],
            dst_ref=zin.at[place, c],
            send_sem=zsend,
            recv_sem=zrecv.at[place, c],
            device_id={"dev": (plane + step) * inner + seat},
            device_id_type=MESH,
        )

    def line_arrival(place, c):
        side = jnp.where(plane > 0, -1, 1)
        return pltpu.make_async_remote_copy(
            src_ref=zout.at[0, c],
            dst_ref=zin.at[place, c],
            send_sem=zsend,
            recv_sem=zrecv.at[place, c],
            device_id={"dev": (plane + side) * inner + seat},
            device_id_type=MESH,
        )

    def aux_copy(j):
        return pltpu.make_async_remote_copy(
            src_ref=zaux.at[j],
            dst_ref=zin_aux.at[plane],
            send_sem=asend,
            recv_sem=arecv,
            device_id={"dev": target_plane(j) * inner + seat},
            device_id_type=MESH,
        )

    def route():
        load_label().wait()
        label = label_ref[...]
        owner = lax.shift_right_logical(label, CL_OWN.bit_length() - 1)
        row = lax.broadcasted_iota(jnp.int32, (LANES, 2 * LANES), 0)
        col = lax.broadcasted_iota(jnp.int32, (LANES, 2 * LANES), 1)
        before = jnp.logical_or(row < col, col >= LANES).astype(jnp.bfloat16)
        index = lax.broadcasted_iota(jnp.int32, (owners, LANES), 0)
        blocks = rows // LANES
        marks = [
            (index == owner[:, b * LANES : (b + 1) * LANES]).astype(jnp.float32)
            for b in range(blocks)
        ]
        counts = jnp.dot(
            jnp.concatenate(marks, axis=0).astype(jnp.bfloat16), before,
            preferred_element_type=jnp.float32,
        )
        running = jnp.zeros((owners, LANES), jnp.float32)
        position = []
        for b in range(blocks):
            block = counts[b * owners : (b + 1) * owners]
            place = marks[b] * (block[:, :LANES] + running)
            position.append(jnp.sum(place, axis=0, keepdims=True))
            running = running + block[:, LANES:]
        position = jnp.concatenate(position, axis=1).astype(jnp.int32)
        inside = owner & (inner - 1)
        swapped = (inside & 1) * 4 + (lax.shift_right_logical(inside, 1) & 1) * 2
        swapped = swapped + lax.shift_right_logical(inside, 2)
        return (owner - inside + swapped) * cap + position

    def picks(j, target):
        row = lax.broadcasted_iota(jnp.int32, (2 * half, 1), 0)
        slot = target_plane(j) * (2 * half) + row
        slot = slot + jnp.where(row < half, core * half, -core * half)
        return (slot == target).astype(jnp.bfloat16)

    def split(c):
        load(c).wait()
        value = stage[c]
        top = value.astype(jnp.bfloat16)
        columns = slice(c * chunk, (c + 1) * chunk)
        high[:, columns] = top
        low[:, columns] = (value - top.astype(jnp.float32)).astype(jnp.bfloat16)
        square = value * value
        square = square[:, :wide] + square[:, wide:]
        if c == 0:
            norm[...] = square
        else:
            norm[...] += square

    def gather(t, pick, begin=0, end=2 * half):
        c = t % chunks
        columns = slice(c * chunk, (c + 1) * chunk)
        if t >= ring and end > half:
            core_copy(t - ring).wait_send()
        rows_of = pick[begin:end]
        block = jnp.dot(rows_of, high[:, columns], preferred_element_type=jnp.float32)
        block = block + jnp.dot(rows_of, low[:, columns], preferred_element_type=jnp.float32)
        for h in range(2):
            part = block[:, h * wide : (h + 1) * wide]
            if begin == 0:
                hold[t, h, :, :, core] = part[:half].reshape(2, 2, cap, wide)
            if end > half:
                cout[t % ring, h] = part[half - begin :].reshape(2, 2, cap, wide)

    def tell():
        norms = jnp.sum(norm[...].T, axis=0, keepdims=True)
        label = (label_ref[...] & (CL_OWN - 1)) + 1
        label = label.astype(jnp.float32).astype(jnp.bfloat16)
        blank = jnp.zeros((4, rows), jnp.bfloat16)
        facts[...] = jnp.concatenate([label] + pieces(norms, 3) + [blank], axis=0)

    def tell_slots(j, pick):
        told = lax.dot_general(
            facts[...], pick, (((1,), (1,)), ((), ())), preferred_element_type=jnp.float32
        )
        told = jnp.concatenate([told[0:1], told[1:2] + told[2:3] + told[3:4]], axis=0)
        for q in range(inner):
            p = q % 2 * 4 + q // 2 % 2 * 2 + (core if q < inner // 2 else 1 - core)
            mine = told[:, q * cap : (q + 1) * cap]
            mout[p, 2 * j : 2 * j + 2] = jnp.concatenate([mine] * rep, axis=1)

    lane = lax.broadcasted_iota(jnp.int32, (8, LANES), 1)
    line = lax.broadcasted_iota(jnp.int32, (8, LANES), 0)
    cluster = lax.broadcasted_iota(jnp.int32, (CL_OWN, LANES), 0).astype(jnp.float32) + 1.0

    def matches(j):
        if j == 0:
            drain(mgot.at[pl.ds(0, inner - 1)], mrecv)
            mgot[seat] = mout[seat]
        weights = []
        for s in range(inner):
            block = mgot[across(s // 2 * 2) - core + s % 2, 2 * j : 2 * j + 2]
            hit[:, s * LANES : (s + 1) * LANES] = (cluster == block[0:1, :]).astype(jnp.bfloat16)
            weight = jnp.where(line == 0, 1.0, 0.0)
            for n, piece in enumerate(pieces(block[1:2, :], 3)):
                weight = jnp.where(line == n + 1, piece.astype(jnp.float32), weight)
            weights.append(jnp.where(lane < cap, weight, 0.0).astype(jnp.bfloat16))
        aux = lax.dot_general(
            jnp.concatenate(weights, axis=1), hit[...], (((1,), (1,)), ((), ())),
            preferred_element_type=jnp.float32,
        )
        if j < last:
            zaux[j] = aux
            aux_copy(j).start()
        else:
            aux_all[...] = aux

    def sources(t, h):
        own = hold.at[t, h, x, y]
        first = xin.at[t, h, y if h == 0 else x]
        direct, passed = yin.at[t, h, 0], yin.at[t, h, 1]
        return (own, first, direct, passed) if h == 0 else (own, direct, first, passed)

    def product(t, h, begin, end):
        stack = []
        for ref in sources(t, h)[begin:end]:
            for s in range(2):
                stack.extend(pieces(ref[s], rep))
        return jnp.dot(
            hit[:, begin * 2 * LANES : end * 2 * LANES], jnp.concatenate(stack, axis=0),
            preferred_element_type=jnp.float32,
        )

    def reduce(j, c):
        t = j * chunks + c
        drain(yin.at[t], yrecv.at[t])
        for h in range(2):
            zout[j, c, :, h * wide : (h + 1) * wide] = product(t, h, 0, 4)

    def conclude(c):
        t = last * chunks + c
        final = t == steps - 1
        if final:
            drain(yin.at[t, :, 0], yrecv.at[steps])
        else:
            drain(yin.at[t], yrecv.at[t])
        for h in range(2):
            total[c, :, h * wide : (h + 1) * wide] = product(t, h, 0, 3 if final else 4)

        @pl.when(plane > 0)
        def _():
            line_arrival(plane, c).wait_recv()
            total[c] += zin[plane, c]

        @pl.when(plane < last)
        def _():
            line_arrival(outer, c).wait_recv()
            total[c] += zin[outer, c]

        if final:
            drain(yin.at[t, :, 1], yrecv.at[t])
        for h in range(2):
            begin = c * chunk + h * wide
            value = total[c, :, h * wide : (h + 1) * wide]
            if final:
                value = value + product(t, h, 3, 4)
            if alone:
                square = value * value
                if c == 0 and h == 0:
                    lengths[...] = square
                else:
                    lengths[...] += square
                value = value * inverse[...]
            main_ref[:, begin : begin + wide] = value

    def forward(j, c):
        @pl.when(fed(j))
        def _():
            line_arrival(target_plane(j), c).wait_recv()
            zout[j, c] += zin[target_plane(j), c]
            line_copy(j, c).start()

    def collect():
        if last:
            drain(zin_aux.at[pl.ds(0, last)], arecv)
        for j in range(last):
            aux_all[...] += zin_aux[target_plane(j)]
        if alone:
            denom = jnp.maximum(aux_all[0:1, :], 1.0)
            inverse[...] = 1.0 / jnp.broadcast_to(denom, (LANES, CL_OWN)).T

    load_label().start()
    load(0).start()
    barrier = pltpu.get_barrier_semaphore()
    for d in range(1, inner):
        peer = plane * inner + across(d)
        pl.semaphore_signal(barrier, inc=1, device_id={"dev": peer}, device_id_type=MESH)
    for d in range(1, outer):
        peer = lax.rem(plane + d, outer) * inner + seat
        pl.semaphore_signal(barrier, inc=1, device_id={"dev": peer}, device_id_type=MESH)

    target = route()
    pick = picks(0, target)
    split(0)
    for c in range(1, chunks):
        load(c).start()
    gather(0, pick, 0, half)
    pl.semaphore_wait(barrier, inner + outer - 2)
    for h in range(2):
        first_copy(0, h, 0).start()
    gather(0, pick, half, 2 * half)
    core_copy(0).start()
    ready = 1

    def prepare(pick):
        nonlocal ready
        t = ready
        if t < steps:
            if t < chunks:
                split(t)
            if t % chunks == 0:
                pick = picks(t // chunks, target)
            gather(t, pick)
            core_copy(t).start()
            ready += 1
        return pick

    split(1)
    gather(1, pick, 0, half)
    for h in range(2):
        first_copy(1, h, 0).start()
    gather(1, pick, half, 2 * half)
    core_copy(1).start()
    ready = 2
    core_arrival(0).wait_recv()
    for h in range(2):
        first_copy(0, h, 1).start()
    for h in range(2):
        direct_copy(0, h).start()
    pick = prepare(pick)
    core_arrival(1).wait_recv()
    for h in range(2):
        first_copy(1, h, 1).start()
    while ready < chunks:
        pick = prepare(pick)
    tell()
    for j in range(outer):
        tell_slots(j, picks(j, target))
    for d in range(1, inner):
        meta_copy(d).start()

    waiting = []

    def arrange(t):
        j, c = t // chunks, t % chunks
        if c == 0:
            matches(j)
        if j == last:
            if c == 0:
                collect()
            conclude(c)
        else:
            reduce(j, c)

            @pl.when(jnp.logical_not(fed(j)))
            def _():
                line_copy(j, c).start()

            if j == last - 1:
                forward(j, c)
            else:
                waiting.append((j, c))
        while waiting and (len(waiting) > 2 or t >= last * chunks - 1):
            forward(*waiting.pop(0))

    for t in range(steps):
        drain(xin.at[t], frecv.at[t])
        for h in range(2):
            passed_copy(t, h).start()
        if t + 2 < steps:
            core_arrival(t + 2).wait_recv()
            for h in range(2):
                first_copy(t + 2, h, 0).start()
        if t + 1 < steps:
            for h in range(2):
                direct_copy(t + 1, h).start()
        pick = prepare(pick)
        if t > 0:
            arrange(t - 1)

    arrange(steps - 1)
    if alone:
        denom = jnp.maximum(aux_all[0:1, :], 1.0)
        squares = aux_all[1:2, :] + aux_all[2:3, :] + aux_all[3:4, :]
        length = jnp.sum(lengths[...].T, axis=0, keepdims=True)
        side_ref[...] = (squares - length / denom) / (denom * width)
    else:
        side_ref[...] = aux_all[...]

    drain(mout.at[pl.ds(0, inner - 1)], msend)
    for t in range(max(steps - ring, 0), steps):
        core_copy(t).wait_send()
    drain(xin, fsend)
    drain(yin, ysend)
    if last:
        drain(zout, zsend)
        drain(zaux, asend)


def body(points, assignment):
    owners = lax.axis_size("dev")
    alone = lax.axis_size("grp") == 1
    rows, width = points.shape
    cap = 2 * rows // owners
    outer = owners // INNER
    chunk = 2 * LANES
    chunks = width // chunk
    wide = chunk // 2
    steps = outer * chunks
    ring = min(steps, 4)

    f32, b16 = jnp.float32, jnp.bfloat16
    dma = pltpu.SemaphoreType.DMA
    hops = max(outer - 1, 1)
    side = (1, CL_OWN) if alone else (8, CL_OWN)
    vmem = pl.BlockSpec(memory_space=pltpu.VMEM)
    hbm = pl.BlockSpec(memory_space=pltpu.HBM)
    main, side = pl.pallas_call(
        functools.partial(kernel, outer, cap, chunk, alone),
        out_shape=(
            jax.ShapeDtypeStruct((CL_OWN, width), f32),
            jax.ShapeDtypeStruct(side, f32),
        ),
        in_specs=[hbm, hbm],
        out_specs=[vmem, vmem],
        scratch_shapes=[
            pltpu.VMEM((1, rows), jnp.int32),
            pltpu.VMEM((chunks, rows, chunk), f32),
            pltpu.VMEM((rows, width), b16),
            pltpu.VMEM((rows, width), b16),
            pltpu.VMEM((rows, LANES), f32),
            pltpu.VMEM((8, rows), b16),
            pltpu.VMEM((CL_OWN, INNER * LANES), b16),
            pltpu.VMEM((steps, 2, 2, 2, 2, cap, wide), f32),
            pltpu.VMEM((ring, 2, 2, 2, cap, wide), f32),
            pltpu.VMEM((steps, 2, 2, 2, cap, wide), f32),
            pltpu.VMEM((steps, 2, 2, 2, cap, wide), f32),
            pltpu.VMEM((INNER, 2 * outer, LANES), f32),
            pltpu.VMEM((INNER, 2 * outer, LANES), f32),
            pltpu.VMEM((hops, chunks, CL_OWN, chunk), f32),
            pltpu.VMEM((outer + 1, chunks, CL_OWN, chunk), f32),
            pltpu.VMEM((hops, 8, CL_OWN), f32),
            pltpu.VMEM((outer, 8, CL_OWN), f32),
            pltpu.VMEM((chunks, CL_OWN, chunk), f32),
            pltpu.VMEM((8, CL_OWN), f32),
            pltpu.VMEM((CL_OWN, LANES), f32),
            pltpu.VMEM((CL_OWN, LANES), f32),
            dma((chunks + 1,)),
            dma(()), dma(()),
            dma((ring,)), dma((steps,)),
            dma(()), dma((steps,)),
            dma(()), dma((steps + 1,)),
            dma(()), dma((outer + 1, chunks)),
            dma(()), dma(()),
        ],
        compiler_params=pltpu.CompilerParams(
            collective_id=0, has_side_effects=True, vmem_limit_bytes=LIMIT
        ),
    )(points, pltpu.with_memory_space_constraint(assignment.reshape(1, rows), pltpu.HBM))
    if alone:
        return main, side[0]
    squares = side[1] + side[2] + side[3]
    sums, counts, squares = lax.psum((main, side[0], squares), "grp")
    return finish(sums, counts, squares)


def solution(mesh):
    return jax.shard_map(
        body,
        mesh=mesh,
        in_specs=(P(("grp", "dev"), None), P(("grp", "dev"))),
        out_specs=(P("dev", None), P("dev")),
        check_vma=False,
    )
```

```python
import functools

import jax
import jax.numpy as jnp
from jax import lax
from jax.experimental import pallas as pl
from jax.experimental.pallas import tpu as pltpu
from jax.sharding import PartitionSpec as P

CL_OWN = 256
LANES = 128
INNER = 8
LIMIT = 52 * 1024 * 1024
MESH = pl.DeviceIdType.MESH


def finish(sums, counts, squares):
    denom = jnp.maximum(counts, 1.0)
    centre = sums / denom[:, None]
    spread = (squares - jnp.sum(sums * sums, axis=1) / denom) / (denom * sums.shape[1])
    return (centre, spread)


def pieces(value, count):
    out = []
    for _ in range(count):
        part = value.astype(jnp.bfloat16)
        out.append(part)
        value = value - part.astype(jnp.float32)
    return out


def kernel(
    outer, cap, chunk, alone, paired,
    points_ref, label_hbm, main_ref, side_ref,
    label_ref, stage, high, low, norm, facts, hit, hold, cout, xin, yin, mout, mgot, zout, zin, zaux, zin_aux,
    total, aux_all, inverse, lengths,
    lsem, msend, mrecv, csend, crecv, fsend, frecv, ysend, yrecv,
    zsend, zrecv, asend, arecv, *extra,
):
    inner = INNER
    me = lax.axis_index("dev")
    plane = me // inner
    seat = lax.rem(me, inner)
    rows, width = points_ref.shape
    owners = inner * outer
    shift = 1 if paired else 0
    chunks = width // chunk - shift
    wide = chunk // 2
    rep = LANES // cap
    last = outer - 1
    rights, lefts = last - plane, plane
    steps = outer * chunks
    half = inner // 2 * cap
    ring = cout.shape[0]
    if paired:
        (
            zlabel, zraw, zhigh, zlow, zfacts, zhold, zcout, zxin, zsout, zsin,
            zzout, zzin, zzown, zmout, zmgot, zhit,
            lssem, lrsem, rssem, rrsem, xcsend, xcrecv, xfsend, xfrecv,
            xssend, xsrecv, zzsend, zzrecv, zmsend, zmrecv,
        ) = extra

    core = lax.rem(seat, 2)
    x = lax.rem(seat // 2, 2)
    y = seat // 4

    def target_plane(j):
        if j == last:
            return plane
        right_first = jnp.where(j < rights, last - j, j - rights)
        left_first = jnp.where(j < lefts, j, last - j + lefts)
        return jnp.where(rights > lefts, right_first, left_first)

    def fed(j):
        k = target_plane(j)
        return jnp.where(k > plane, plane > 0, plane < last)

    def across(d):
        other = 0
        for bit in range(3):
            own = lax.rem(seat // 2**bit, 2)
            other = other + (1 - own if d // 2**bit % 2 else own) * 2**bit
        return other

    def load_label():
        return pltpu.make_async_copy(label_hbm, label_ref, lsem.at[width // chunk])

    def load(c):
        return pltpu.make_async_copy(
            points_ref.at[:, pl.ds(c * chunk, chunk)], stage.at[c], lsem.at[c]
        )

    def drain(ref, sem):
        pltpu.make_async_copy(ref, ref, sem).wait()

    def plane_copy(src, dst, ssem, rsem, d):
        return pltpu.make_async_remote_copy(
            src_ref=src,
            dst_ref=dst,
            send_sem=ssem,
            recv_sem=rsem,
            device_id={"dev": plane * inner + across(d)},
            device_id_type=MESH,
        )

    def core_copy(t):
        return plane_copy(
            cout.at[t % ring], hold.at[t, :, :, :, core], csend.at[t % ring], crecv.at[t], 1
        )

    def core_arrival(t):
        return plane_copy(
            cout.at[t % ring], hold.at[t, :, :, :, 1 - core], csend.at[t % ring], crecv.at[t], 1
        )

    def parts_of(t):
        return 2 if t < 2 else 1

    def first_copy(t, h, part):
        source = hold.at[t, 0, 1 - x] if h == 0 else hold.at[t, 1, :, 1 - y]
        target = xin.at[t, h]
        if parts_of(t) == 2:
            of = core if part == 0 else 1 - core
            source = hold.at[t, 0, 1 - x, :, of] if h == 0 else hold.at[t, 1, :, 1 - y, of]
            target = xin.at[t, h, :, of]
        return plane_copy(source, target, fsend, frecv.at[t], 2 if h == 0 else 4)

    def direct_copy(t, h):
        source = hold.at[t, 0, x, 1 - y] if h == 0 else hold.at[t, 1, 1 - x, y]
        arrived = yrecv.at[steps if t == steps - 1 else t]
        return plane_copy(source, yin.at[t, h, 0], ysend, arrived, 4 if h == 0 else 2)

    def passed_copy(t, h):
        source = xin.at[t, 0, 1 - y] if h == 0 else xin.at[t, 1, 1 - x]
        return plane_copy(source, yin.at[t, h, 1], ysend, yrecv.at[t], 4 if h == 0 else 2)

    def meta_copy(d):
        return plane_copy(mout.at[across(d)], mgot.at[seat], msend, mrecv, d)

    def line_copy(j, c):
        k = target_plane(j)
        step = jnp.where(k > plane, 1, -1)
        place = jnp.where(k == plane - 1, outer, k)
        return pltpu.make_async_remote_copy(
            src_ref=zout.at[j, c],
            dst_ref=zin.at[place, c],
            send_sem=zsend,
            recv_sem=zrecv.at[place, c],
            device_id={"dev": (plane + step) * inner + seat},
            device_id_type=MESH,
        )

    def line_arrival(place, c):
        side = jnp.where(plane > 0, -1, 1)
        return pltpu.make_async_remote_copy(
            src_ref=zout.at[0, c],
            dst_ref=zin.at[place, c],
            send_sem=zsend,
            recv_sem=zrecv.at[place, c],
            device_id={"dev": (plane + side) * inner + seat},
            device_id_type=MESH,
        )

    def aux_copy(j):
        return pltpu.make_async_remote_copy(
            src_ref=zaux.at[j],
            dst_ref=zin_aux.at[plane],
            send_sem=asend,
            recv_sem=arecv,
            device_id={"dev": target_plane(j) * inner + seat},
            device_id_type=MESH,
        )

    def route(label):
        owner = lax.shift_right_logical(label, CL_OWN.bit_length() - 1)
        row = lax.broadcasted_iota(jnp.int32, (LANES, 2 * LANES), 0)
        col = lax.broadcasted_iota(jnp.int32, (LANES, 2 * LANES), 1)
        before = jnp.logical_or(row < col, col >= LANES).astype(jnp.bfloat16)
        index = lax.broadcasted_iota(jnp.int32, (owners, LANES), 0)
        blocks = rows // LANES
        marks = [
            (index == owner[:, b * LANES : (b + 1) * LANES]).astype(jnp.float32)
            for b in range(blocks)
        ]
        counts = jnp.dot(
            jnp.concatenate(marks, axis=0).astype(jnp.bfloat16), before,
            preferred_element_type=jnp.float32,
        )
        running = jnp.zeros((owners, LANES), jnp.float32)
        position = []
        for b in range(blocks):
            block = counts[b * owners : (b + 1) * owners]
            place = marks[b] * (block[:, :LANES] + running)
            position.append(jnp.sum(place, axis=0, keepdims=True))
            running = running + block[:, LANES:]
        position = jnp.concatenate(position, axis=1).astype(jnp.int32)
        inside = owner & (inner - 1)
        swapped = (inside & 1) * 4 + (lax.shift_right_logical(inside, 1) & 1) * 2
        swapped = swapped + lax.shift_right_logical(inside, 2)
        return (owner - inside + swapped) * cap + position

    def picks(k, target):
        row = lax.broadcasted_iota(jnp.int32, (2 * half, 1), 0)
        slot = k * (2 * half) + row
        slot = slot + jnp.where(row < half, core * half, -core * half)
        return (slot == target).astype(jnp.bfloat16)

    def split(c):
        load(c).wait()
        value = stage[c]
        top = value.astype(jnp.bfloat16)
        columns = slice(c * chunk, (c + 1) * chunk)
        high[:, columns] = top
        low[:, columns] = (value - top.astype(jnp.float32)).astype(jnp.bfloat16)
        square = value * value
        square = square[:, :wide] + square[:, wide:]
        if c == shift:
            norm[...] = square
        else:
            norm[...] += square

    def gather(t, pick, begin=0, end=2 * half):
        c = t % chunks + shift
        columns = slice(c * chunk, (c + 1) * chunk)
        if t >= ring and end > half:
            core_copy(t - ring).wait_send()
        rows_of = pick[begin:end]
        block = jnp.dot(rows_of, high[:, columns], preferred_element_type=jnp.float32)
        block = block + jnp.dot(rows_of, low[:, columns], preferred_element_type=jnp.float32)
        for h in range(2):
            part = block[:, h * wide : (h + 1) * wide]
            if begin == 0:
                hold[t, h, :, :, core] = part[:half].reshape(2, 2, cap, wide)
            if end > half:
                cout[t % ring, h] = part[half - begin :].reshape(2, 2, cap, wide)

    def inside_label(label):
        return ((label & (CL_OWN - 1)) + 1).astype(jnp.float32).astype(jnp.bfloat16)

    def tell():
        norms = jnp.sum(norm[...].T, axis=0, keepdims=True)
        label = inside_label(label_ref[...])
        blank = jnp.zeros((4, rows), jnp.bfloat16)
        facts[...] = jnp.concatenate([label] + pieces(norms, 3) + [blank], axis=0)

    def tell_slots(j, pick):
        told = lax.dot_general(
            facts[...], pick, (((1,), (1,)), ((), ())), preferred_element_type=jnp.float32
        )
        told = jnp.concatenate([told[0:1], told[1:2] + told[2:3] + told[3:4]], axis=0)
        for q in range(inner):
            p = q % 2 * 4 + q // 2 % 2 * 2 + (core if q < inner // 2 else 1 - core)
            mine = told[:, q * cap : (q + 1) * cap]
            mout[p, 2 * j : 2 * j + 2] = jnp.concatenate([mine] * rep, axis=1)

    lane = lax.broadcasted_iota(jnp.int32, (8, LANES), 1)
    line = lax.broadcasted_iota(jnp.int32, (8, LANES), 0)
    cluster = lax.broadcasted_iota(jnp.int32, (CL_OWN, LANES), 0).astype(jnp.float32) + 1.0

    def matches(j):
        if j == 0:
            drain(mgot.at[pl.ds(0, inner - 1)], mrecv)
            mgot[seat] = mout[seat]
        weights = []
        for s in range(inner):
            block = mgot[across(s // 2 * 2) - core + s % 2, 2 * j : 2 * j + 2]
            hit[:, s * LANES : (s + 1) * LANES] = (cluster == block[0:1, :]).astype(jnp.bfloat16)
            weight = jnp.where(line == 0, 1.0, 0.0)
            for n, piece in enumerate(pieces(block[1:2, :], 3)):
                weight = jnp.where(line == n + 1, piece.astype(jnp.float32), weight)
            weights.append(jnp.where(lane < cap, weight, 0.0).astype(jnp.bfloat16))
        aux = lax.dot_general(
            jnp.concatenate(weights, axis=1), hit[...], (((1,), (1,)), ((), ())),
            preferred_element_type=jnp.float32,
        )
        if j < last:
            zaux[j] = aux
            aux_copy(j).start()
        else:
            aux_all[...] = aux

    def sources(t, h):
        own = hold.at[t, h, x, y]
        first = xin.at[t, h, y if h == 0 else x]
        direct, passed = yin.at[t, h, 0], yin.at[t, h, 1]
        return (own, first, direct, passed) if h == 0 else (own, direct, first, passed)

    def product(t, h, begin, end):
        stack = []
        for ref in sources(t, h)[begin:end]:
            for s in range(2):
                stack.extend(pieces(ref[s], rep))
        return jnp.dot(
            hit[:, begin * 2 * LANES : end * 2 * LANES], jnp.concatenate(stack, axis=0),
            preferred_element_type=jnp.float32,
        )

    def reduce(j, c):
        t = j * chunks + c
        drain(yin.at[t], yrecv.at[t])
        for h in range(2):
            zout[j, c, :, h * wide : (h + 1) * wide] = product(t, h, 0, 4)

    def conclude(c):
        t = last * chunks + c
        final = t == steps - 1
        if final:
            drain(yin.at[t, :, 0], yrecv.at[steps])
        else:
            drain(yin.at[t], yrecv.at[t])
        for h in range(2):
            total[c, :, h * wide : (h + 1) * wide] = product(t, h, 0, 3 if final else 4)

        @pl.when(plane > 0)
        def _():
            line_arrival(plane, c).wait_recv()
            total[c] += zin[plane, c]

        @pl.when(plane < last)
        def _():
            line_arrival(outer, c).wait_recv()
            total[c] += zin[outer, c]

        if final:
            drain(yin.at[t, :, 1], yrecv.at[t])
        for h in range(2):
            begin = (c + shift) * chunk + h * wide
            value = total[c, :, h * wide : (h + 1) * wide]
            if final:
                value = value + product(t, h, 3, 4)
            if alone:
                square = value * value
                if c == 0 and h == 0:
                    lengths[...] = square
                else:
                    lengths[...] += square
                value = value * inverse[...]
            main_ref[:, begin : begin + wide] = value

    def forward(j, c):
        @pl.when(fed(j))
        def _():
            line_arrival(target_plane(j), c).wait_recv()
            zout[j, c] += zin[target_plane(j), c]
            line_copy(j, c).start()

    def collect():
        if last:
            drain(zin_aux.at[pl.ds(0, last)], arecv)
        for j in range(last):
            aux_all[...] += zin_aux[target_plane(j)]
        if alone:
            denom = jnp.maximum(aux_all[0:1, :], 1.0)
            inverse[...] = 1.0 / jnp.broadcast_to(denom, (LANES, CL_OWN)).T

    def pair_copy(src, dst, ssem, rsem):
        return pltpu.make_async_remote_copy(
            src_ref=src,
            dst_ref=dst,
            send_sem=ssem,
            recv_sem=rsem,
            device_id={"dev": (plane + 1 - 2 * lax.rem(plane, 2)) * inner + seat},
            device_id_type=MESH,
        )

    def pair_label():
        return pair_copy(label_hbm, zlabel, lssem, lrsem)

    def pair_rows():
        return pair_copy(points_ref.at[:, pl.ds(0, chunk)], zraw, rssem, rrsem)

    def pair_plane(m):
        return lax.rem(plane + 2, outer) if m == 0 else plane

    def pair_tell(pair_target):
        zfacts[...] = jnp.concatenate(
            [inside_label(zlabel[...]), jnp.zeros((7, rows), jnp.bfloat16)], axis=0
        )
        for m in range(2):
            for zs, (fact, slots) in enumerate(((facts, target), (zfacts, pair_target))):
                told = lax.dot_general(
                    fact[...], picks(pair_plane(m), slots), (((1,), (1,)), ((), ())),
                    preferred_element_type=jnp.float32,
                )
                for side in range(2):
                    for xx in range(2):
                        row = m * 4 + zs * 2 + xx
                        begin = side * half + xx * LANES
                        zmout[side, row : row + 1] = told[0:1, begin : begin + LANES]
        zmgot[core] = zmout[0]
        for d in range(1, 6):
            plane_copy(zmout.at[d % 2], zmgot.at[d // 2 * 2 + core], zmsend, zmrecv, d).start()

    def pair_core(m, zs):
        return plane_copy(
            zcout.at[m, zs], zhold.at[m, :, :, :, zs * 2 + core], xcsend, xcrecv.at[m], 1
        )

    def pair_first(m, h):
        source = zhold.at[m, 0, 1 - x] if h == 0 else zhold.at[m, 1, :, 1 - y]
        return plane_copy(source, zxin.at[m, h], xfsend, xfrecv.at[m], 2 if h == 0 else 4)

    def pair_sums(m, h):
        return plane_copy(
            zsout.at[m, h], zsin.at[m, h], xssend, xsrecv.at[m], 4 if h == 0 else 2
        )

    def pair_line():
        return pltpu.make_async_remote_copy(
            src_ref=zzout,
            dst_ref=zzin,
            send_sem=zzsend,
            recv_sem=zzrecv,
            device_id={"dev": pair_plane(0) * inner + seat},
            device_id_type=MESH,
        )

    def pair_gather(m, pair_target):
        if m == 0:
            pair_rows().wait_recv()
            value = zraw[...]
            top = value.astype(jnp.bfloat16)
            zhigh[...] = top
            zlow[...] = (value - top.astype(jnp.float32)).astype(jnp.bfloat16)
        for zs in range(2):
            pick = picks(pair_plane(m), pair_target if zs else target)
            upper = zhigh[...] if zs else high[:, :chunk]
            lower = zlow[...] if zs else low[:, :chunk]
            block = jnp.dot(pick, upper, preferred_element_type=jnp.float32)
            block = block + jnp.dot(pick, lower, preferred_element_type=jnp.float32)
            for h in range(2):
                part = block[:, h * wide : (h + 1) * wide]
                zhold[m, h, :, :, zs * 2 + core] = part[:half].reshape(2, 2, cap, wide)
                zcout[m, zs, h] = part[half:].reshape(2, 2, cap, wide)
            pair_core(m, zs).start()

    def pair_product(m, h, away):
        xx = 1 - x if away and h == 1 else x
        yy = 1 - y if away and h == 0 else y
        stack = []
        for side, ref in enumerate((zhold.at[m, h, xx, yy], zxin.at[m, h, yy if h == 0 else xx])):
            for s in range(4):
                got = zmgot[(1 + h) * 2 * side + s % 2, pl.ds(m * 4 + s // 2 * 2 + xx, 1)]
                label = jnp.where(
                    yy == 1,
                    jnp.concatenate([got[:, cap:]] * 2, axis=1),
                    jnp.concatenate([got[:, :cap]] * 2, axis=1),
                )
                n = side * 4 + s
                zhit[:, n * LANES : (n + 1) * LANES] = (cluster == label).astype(jnp.bfloat16)
                stack.extend(pieces(ref[s], rep))
        return jnp.dot(
            zhit[...], jnp.concatenate(stack, axis=0), preferred_element_type=jnp.float32
        )

    def pair_send(m):
        if m == 0:
            drain(zmgot.at[pl.ds(0, 5)], zmrecv)
        for h in range(2):
            zsout[m, h] = pair_product(m, h, True)
            pair_sums(m, h).start()

    def pair_arrange(m):
        for h in range(2):
            columns = slice(h * wide, (h + 1) * wide)
            own = zzout if m == 0 else zzown
            own[:, columns] = pair_product(m, h, False)
        drain(zsin.at[m], xsrecv.at[m])
        for h in range(2):
            columns = slice(h * wide, (h + 1) * wide)
            own = zzout if m == 0 else zzown
            own[:, columns] += zsin[m, h]
        if m == 0:
            pair_line().start()

    def pair_conclude():
        pair_line().wait_recv()
        for h in range(2):
            columns = slice(h * wide, (h + 1) * wide)
            value = zzown[:, columns] + zzin[:, columns]
            if alone:
                lengths[...] += value * value
                value = value * inverse[...]
            main_ref[:, columns] = value

    load_label().start()
    load(shift).start()
    barrier = pltpu.get_barrier_semaphore()
    for d in range(1, inner):
        peer = plane * inner + across(d)
        pl.semaphore_signal(barrier, inc=1, device_id={"dev": peer}, device_id_type=MESH)
    for d in range(1, outer):
        peer = lax.rem(plane + d, outer) * inner + seat
        pl.semaphore_signal(barrier, inc=1, device_id={"dev": peer}, device_id_type=MESH)

    load_label().wait()
    target = route(label_ref[...])
    pick = picks(target_plane(0), target)
    split(shift)
    for c in range(width // chunk):
        if c != shift:
            load(c).start()
    gather(0, pick, 0, half)
    pl.semaphore_wait(barrier, inner + outer - 2)
    for h in range(2):
        first_copy(0, h, 0).start()
    if paired:
        pair_label().start()
        pair_rows().start()
    gather(0, pick, half, 2 * half)
    core_copy(0).start()

    def prepare(t):
        nonlocal pick
        if t < chunks:
            split(t + shift)
        if t % chunks == 0:
            pick = picks(target_plane(t // chunks), target)
        gather(t, pick)
        core_copy(t).start()

    def push(t):
        core_arrival(t).wait_recv()
        for h in range(2):
            first_copy(t, h, parts_of(t) - 1).start()

    def pair_push(m):
        drain(zcout.at[m], xcrecv.at[m])
        for h in range(2):
            pair_first(m, h).start()

    def direct(t):
        for h in range(2):
            direct_copy(t, h).start()

    def head(t):
        drain(xin.at[t], frecv.at[t])
        for h in range(2):
            passed_copy(t, h).start()

    def arrange(t):
        j, c = t // chunks, t % chunks
        if c == 0:
            matches(j)
        if j == last:
            if c == 0:
                collect()
            conclude(c)
            return
        reduce(j, c)

        @pl.when(jnp.logical_not(fed(j)))
        def _():
            line_copy(j, c).start()

    split(1 + shift)
    gather(1, pick, 0, half)
    for h in range(2):
        first_copy(1, h, 0).start()
    gather(1, pick, half, 2 * half)
    core_copy(1).start()
    push(0)
    direct(0)
    prepare(2)
    push(1)
    if paired:
        split(0)
    tell()
    for j in range(outer - 1):
        tell_slots(j, picks(target_plane(j), target))
    head(0)
    tell_slots(last, picks(target_plane(last), target))
    for d in range(1, inner):
        meta_copy(d).start()
    push(2)
    direct(1)
    prepare(3)

    if paired:
        head(1)
        push(3)
        direct(2)
        pair_label().wait_recv()
        pair_target = route(zlabel[...])
        pair_tell(pair_target)
        prepare(4)
        arrange(0)

        head(2)
        push(4)
        direct(3)
        prepare(5)
        arrange(1)

        head(3)
        push(5)
        direct(4)
        arrange(2)
        pair_gather(0, pair_target)

        head(4)
        pair_push(0)
        direct(5)
        prepare(6)
        arrange(3)

        head(5)
        forward(0, 0)
        pair_gather(1, pair_target)
        arrange(4)
        forward(0, 1)
        pair_push(1)

        drain(zxin.at[0], xfrecv.at[0])
        pair_send(0)
        push(6)
        prepare(7)
        forward(2, 0)
        arrange(5)
        forward(1, 0)
        forward(2, 1)

        drain(zxin.at[1], xfrecv.at[1])
        pair_send(1)
        push(7)
        direct(6)
        forward(1, 1)
        pair_arrange(0)

        head(6)
        direct(7)
        pair_arrange(1)

        head(7)
        arrange(6)
        arrange(7)
        pair_conclude()
    else:
        waiting = []
        for t in range(1, steps + 1):
            if t < steps:
                head(t)
            if t + 2 < steps:
                push(t + 2)
            if t + 1 < steps:
                direct(t + 1)
            if t + 3 < steps:
                prepare(t + 3)
            arrange(t - 1)
            j, c = (t - 1) // chunks, (t - 1) % chunks
            if j == last - 1:
                forward(j, c)
            elif j < last:
                waiting.append((j, c))
            while waiting and (len(waiting) > 2 or t >= last * chunks):
                forward(*waiting.pop(0))
    if alone:
        denom = jnp.maximum(aux_all[0:1, :], 1.0)
        squares = aux_all[1:2, :] + aux_all[2:3, :] + aux_all[3:4, :]
        length = jnp.sum(lengths[...].T, axis=0, keepdims=True)
        side_ref[...] = (squares - length / denom) / (denom * width)
    else:
        side_ref[...] = aux_all[...]

    drain(mout.at[pl.ds(0, inner - 1)], msend)
    for t in range(max(steps - ring, 0), steps):
        core_copy(t).wait_send()
    drain(xin, fsend)
    drain(yin, ysend)
    if last:
        drain(zout, zsend)
        drain(zaux, asend)
    if paired:
        pair_label().wait_send()
        pair_rows().wait_send()
        drain(zmgot.at[pl.ds(0, 5)], zmsend)
        drain(zcout, xcsend)
        drain(zxin, xfsend)
        drain(zsout, xssend)
        pair_line().wait_send()


def body(points, assignment):
    owners = lax.axis_size("dev")
    alone = lax.axis_size("grp") == 1
    rows, width = points.shape
    cap = 2 * rows // owners
    outer = owners // INNER
    chunk = 2 * LANES
    paired = outer == 4 and 2 * cap == LANES and width == 3 * chunk
    chunks = width // chunk - (1 if paired else 0)
    wide = chunk // 2
    steps = outer * chunks
    ring = min(steps, 4)

    f32, b16 = jnp.float32, jnp.bfloat16
    dma = pltpu.SemaphoreType.DMA
    hops = max(outer - 1, 1)
    side = (1, CL_OWN) if alone else (8, CL_OWN)
    extra = [
        pltpu.VMEM((1, rows), jnp.int32),
        pltpu.VMEM((rows, chunk), f32),
        pltpu.VMEM((rows, chunk), b16),
        pltpu.VMEM((rows, chunk), b16),
        pltpu.VMEM((8, rows), b16),
        pltpu.VMEM((2, 2, 2, 2, 4, cap, wide), f32),
        pltpu.VMEM((2, 2, 2, 2, 2, cap, wide), f32),
        pltpu.VMEM((2, 2, 2, 4, cap, wide), f32),
        pltpu.VMEM((2, 2, CL_OWN, wide), f32),
        pltpu.VMEM((2, 2, CL_OWN, wide), f32),
        pltpu.VMEM((CL_OWN, chunk), f32),
        pltpu.VMEM((CL_OWN, chunk), f32),
        pltpu.VMEM((CL_OWN, chunk), f32),
        pltpu.VMEM((2, 8, LANES), f32),
        pltpu.VMEM((6, 8, LANES), f32),
        pltpu.VMEM((CL_OWN, INNER * LANES), b16),
        dma(()), dma(()), dma(()), dma(()),
        dma(()), dma((2,)), dma(()), dma((2,)),
        dma(()), dma((2,)), dma(()), dma(()), dma(()), dma(()),
    ]
    vmem = pl.BlockSpec(memory_space=pltpu.VMEM)
    hbm = pl.BlockSpec(memory_space=pltpu.HBM)
    main, side = pl.pallas_call(
        functools.partial(kernel, outer, cap, chunk, alone, paired),
        out_shape=(
            jax.ShapeDtypeStruct((CL_OWN, width), f32),
            jax.ShapeDtypeStruct(side, f32),
        ),
        in_specs=[hbm, hbm],
        out_specs=[vmem, vmem],
        scratch_shapes=[
            pltpu.VMEM((1, rows), jnp.int32),
            pltpu.VMEM((width // chunk, rows, chunk), f32),
            pltpu.VMEM((rows, width), b16),
            pltpu.VMEM((rows, width), b16),
            pltpu.VMEM((rows, LANES), f32),
            pltpu.VMEM((8, rows), b16),
            pltpu.VMEM((CL_OWN, INNER * LANES), b16),
            pltpu.VMEM((steps, 2, 2, 2, 2, cap, wide), f32),
            pltpu.VMEM((ring, 2, 2, 2, cap, wide), f32),
            pltpu.VMEM((steps, 2, 2, 2, cap, wide), f32),
            pltpu.VMEM((steps, 2, 2, 2, cap, wide), f32),
            pltpu.VMEM((INNER, 2 * outer, LANES), f32),
            pltpu.VMEM((INNER, 2 * outer, LANES), f32),
            pltpu.VMEM((hops, chunks, CL_OWN, chunk), f32),
            pltpu.VMEM((outer + 1, chunks, CL_OWN, chunk), f32),
            pltpu.VMEM((hops, 8, CL_OWN), f32),
            pltpu.VMEM((outer, 8, CL_OWN), f32),
            pltpu.VMEM((chunks, CL_OWN, chunk), f32),
            pltpu.VMEM((8, CL_OWN), f32),
            pltpu.VMEM((CL_OWN, LANES), f32),
            pltpu.VMEM((CL_OWN, LANES), f32),
            dma((width // chunk + 1,)),
            dma(()), dma(()),
            dma((ring,)), dma((steps,)),
            dma(()), dma((steps,)),
            dma(()), dma((steps + 1,)),
            dma(()), dma((outer + 1, chunks)),
            dma(()), dma(()),
        ] + (extra if paired else []),
        compiler_params=pltpu.CompilerParams(
            collective_id=0, has_side_effects=True, vmem_limit_bytes=LIMIT
        ),
    )(points, pltpu.with_memory_space_constraint(assignment.reshape(1, rows), pltpu.HBM))
    if alone:
        return main, side[0]
    squares = side[1] + side[2] + side[3]
    sums, counts, squares = lax.psum((main, side[0], squares), "grp")
    return finish(sums, counts, squares)


def solution(mesh):
    return jax.shard_map(
        body,
        mesh=mesh,
        in_specs=(P(("grp", "dev"), None), P(("grp", "dev"))),
        out_specs=(P("dev", None), P("dev")),
        check_vma=False,
    )
```

```python
import functools

import jax
import jax.numpy as jnp
from jax import lax
from jax.experimental import pallas as pl
from jax.experimental.pallas import tpu as pltpu
from jax.sharding import PartitionSpec as P

CL_OWN = 256
LANES = 128
INNER = 8
LIMIT = 52 * 1024 * 1024
MESH = pl.DeviceIdType.MESH


def finish(sums, counts, squares):
    denom = jnp.maximum(counts, 1.0)
    centre = sums / denom[:, None]
    spread = (squares - jnp.sum(sums * sums, axis=1) / denom) / (denom * sums.shape[1])
    return (centre, spread)


def pieces(value, count):
    out = []
    for _ in range(count):
        part = value.astype(jnp.bfloat16)
        out.append(part)
        value = value - part.astype(jnp.float32)
    return out


def kernel(
    outer, cap, chunk, alone, paired,
    points_ref, label_hbm, main_ref, side_ref,
    label_ref, stage, high, low, norm, facts, hit, hold, cout, xin, yin, mout, mgot, zout, zin, zaux, zin_aux,
    total, aux_all, inverse, lengths,
    lsem, msend, mrecv, csend, crecv, fsend, frecv, ysend, yrecv,
    zsend, zrecv, asend, arecv, *extra,
):
    inner = INNER
    me = lax.axis_index("dev")
    plane = me // inner
    seat = lax.rem(me, inner)
    rows, width = points_ref.shape
    owners = inner * outer
    shift = 1 if paired else 0
    chunks = width // chunk - shift
    wide = chunk // 2
    rep = LANES // cap
    last = outer - 1
    rights, lefts = last - plane, plane
    steps = outer * chunks
    half = inner // 2 * cap
    ring = cout.shape[0]
    if paired:
        (
            zlabel, zraw, zhigh, zlow, zfacts, zhold, zcout, zxin, zsout, zsin,
            zzout, zzin, zzown, zmout, zmgot, zhit,
            lssem, lrsem, rssem, rrsem, xcsend, xcrecv, xfsend, xfrecv,
            xssend, xsrecv, zzsend, zzrecv, zmsend, zmrecv,
        ) = extra

    core = lax.rem(seat, 2)
    x = lax.rem(seat // 2, 2)
    y = seat // 4

    def target_plane(j):
        if j == last:
            return plane
        right_first = jnp.where(j < rights, last - j, j - rights)
        left_first = jnp.where(j < lefts, j, last - j + lefts)
        return jnp.where(rights > lefts, right_first, left_first)

    def fed(j):
        k = target_plane(j)
        return jnp.where(k > plane, plane > 0, plane < last)

    def across(d):
        other = 0
        for bit in range(3):
            own = lax.rem(seat // 2**bit, 2)
            other = other + (1 - own if d // 2**bit % 2 else own) * 2**bit
        return other

    def load_label():
        return pltpu.make_async_copy(label_hbm, label_ref, lsem.at[width // chunk])

    def load(c):
        return pltpu.make_async_copy(
            points_ref.at[:, pl.ds(c * chunk, chunk)], stage.at[c], lsem.at[c]
        )

    def drain(ref, sem):
        pltpu.make_async_copy(ref, ref, sem).wait()

    def plane_copy(src, dst, ssem, rsem, d):
        return pltpu.make_async_remote_copy(
            src_ref=src,
            dst_ref=dst,
            send_sem=ssem,
            recv_sem=rsem,
            device_id={"dev": plane * inner + across(d)},
            device_id_type=MESH,
        )

    def core_copy(t):
        return plane_copy(
            cout.at[t % ring], hold.at[t, :, :, :, core], csend.at[t % ring], crecv.at[t], 1
        )

    def core_arrival(t):
        return plane_copy(
            cout.at[t % ring], hold.at[t, :, :, :, 1 - core], csend.at[t % ring], crecv.at[t], 1
        )

    def parts_of(t):
        return 2 if t < 2 else 1

    def first_copy(t, h, part):
        source = hold.at[t, 0, 1 - x] if h == 0 else hold.at[t, 1, :, 1 - y]
        target = xin.at[t, h]
        if parts_of(t) == 2:
            of = core if part == 0 else 1 - core
            source = hold.at[t, 0, 1 - x, :, of] if h == 0 else hold.at[t, 1, :, 1 - y, of]
            target = xin.at[t, h, :, of]
        return plane_copy(source, target, fsend, frecv.at[t], 2 if h == 0 else 4)

    def direct_copy(t, h):
        source = hold.at[t, 0, x, 1 - y] if h == 0 else hold.at[t, 1, 1 - x, y]
        arrived = yrecv.at[steps if t == steps - 1 else t]
        return plane_copy(source, yin.at[t, h, 0], ysend, arrived, 4 if h == 0 else 2)

    def passed_copy(t, h):
        source = xin.at[t, 0, 1 - y] if h == 0 else xin.at[t, 1, 1 - x]
        return plane_copy(source, yin.at[t, h, 1], ysend, yrecv.at[t], 4 if h == 0 else 2)

    def meta_copy(d):
        return plane_copy(mout.at[across(d)], mgot.at[seat], msend, mrecv, d)

    def line_copy(j, c):
        k = target_plane(j)
        step = jnp.where(k > plane, 1, -1)
        place = jnp.where(k == plane - 1, outer, k)
        return pltpu.make_async_remote_copy(
            src_ref=zout.at[j, c],
            dst_ref=zin.at[place, c],
            send_sem=zsend,
            recv_sem=zrecv.at[place, c],
            device_id={"dev": (plane + step) * inner + seat},
            device_id_type=MESH,
        )

    def line_arrival(place, c):
        side = jnp.where(plane > 0, -1, 1)
        return pltpu.make_async_remote_copy(
            src_ref=zout.at[0, c],
            dst_ref=zin.at[place, c],
            send_sem=zsend,
            recv_sem=zrecv.at[place, c],
            device_id={"dev": (plane + side) * inner + seat},
            device_id_type=MESH,
        )

    def aux_copy(j):
        return pltpu.make_async_remote_copy(
            src_ref=zaux.at[j],
            dst_ref=zin_aux.at[plane],
            send_sem=asend,
            recv_sem=arecv,
            device_id={"dev": target_plane(j) * inner + seat},
            device_id_type=MESH,
        )

    def route(label):
        owner = lax.shift_right_logical(label, CL_OWN.bit_length() - 1)
        row = lax.broadcasted_iota(jnp.int32, (LANES, 2 * LANES), 0)
        col = lax.broadcasted_iota(jnp.int32, (LANES, 2 * LANES), 1)
        before = jnp.logical_or(row < col, col >= LANES).astype(jnp.bfloat16)
        index = lax.broadcasted_iota(jnp.int32, (owners, LANES), 0)
        blocks = rows // LANES
        marks = [
            (index == owner[:, b * LANES : (b + 1) * LANES]).astype(jnp.float32)
            for b in range(blocks)
        ]
        counts = jnp.dot(
            jnp.concatenate(marks, axis=0).astype(jnp.bfloat16), before,
            preferred_element_type=jnp.float32,
        )
        running = jnp.zeros((owners, LANES), jnp.float32)
        position = []
        for b in range(blocks):
            block = counts[b * owners : (b + 1) * owners]
            place = marks[b] * (block[:, :LANES] + running)
            position.append(jnp.sum(place, axis=0, keepdims=True))
            running = running + block[:, LANES:]
        position = jnp.concatenate(position, axis=1).astype(jnp.int32)
        inside = owner & (inner - 1)
        swapped = (inside & 1) * 4 + (lax.shift_right_logical(inside, 1) & 1) * 2
        swapped = swapped + lax.shift_right_logical(inside, 2)
        return (owner - inside + swapped) * cap + position

    def picks(k, target):
        row = lax.broadcasted_iota(jnp.int32, (2 * half, 1), 0)
        slot = k * (2 * half) + row
        slot = slot + jnp.where(row < half, core * half, -core * half)
        return (slot == target).astype(jnp.bfloat16)

    def split(c):
        load(c).wait()
        value = stage[c]
        top = value.astype(jnp.bfloat16)
        columns = slice(c * chunk, (c + 1) * chunk)
        high[:, columns] = top
        low[:, columns] = (value - top.astype(jnp.float32)).astype(jnp.bfloat16)
        square = value * value
        square = square[:, :wide] + square[:, wide:]
        if c == shift:
            norm[...] = square
        else:
            norm[...] += square

    def gather(t, pick, begin=0, end=2 * half):
        c = t % chunks + shift
        columns = slice(c * chunk, (c + 1) * chunk)
        if t >= ring and end > half:
            core_copy(t - ring).wait_send()
        rows_of = pick[begin:end]
        block = jnp.dot(rows_of, high[:, columns], preferred_element_type=jnp.float32)
        block = block + jnp.dot(rows_of, low[:, columns], preferred_element_type=jnp.float32)
        for h in range(2):
            part = block[:, h * wide : (h + 1) * wide]
            if begin == 0:
                hold[t, h, :, :, core] = part[:half].reshape(2, 2, cap, wide)
            if end > half:
                cout[t % ring, h] = part[half - begin :].reshape(2, 2, cap, wide)

    def inside_label(label):
        return ((label & (CL_OWN - 1)) + 1).astype(jnp.float32).astype(jnp.bfloat16)

    def tell():
        norms = jnp.sum(norm[...].T, axis=0, keepdims=True)
        label = inside_label(label_ref[...])
        blank = jnp.zeros((4, rows), jnp.bfloat16)
        facts[...] = jnp.concatenate([label] + pieces(norms, 3) + [blank], axis=0)

    def tell_slots(j, pick):
        told = lax.dot_general(
            facts[...], pick, (((1,), (1,)), ((), ())), preferred_element_type=jnp.float32
        )
        told = jnp.concatenate([told[0:1], told[1:2] + told[2:3] + told[3:4]], axis=0)
        for q in range(inner):
            p = q % 2 * 4 + q // 2 % 2 * 2 + (core if q < inner // 2 else 1 - core)
            mine = told[:, q * cap : (q + 1) * cap]
            mout[p, 2 * j : 2 * j + 2] = jnp.concatenate([mine] * rep, axis=1)

    lane = lax.broadcasted_iota(jnp.int32, (8, LANES), 1)
    line = lax.broadcasted_iota(jnp.int32, (8, LANES), 0)
    cluster = lax.broadcasted_iota(jnp.int32, (CL_OWN, LANES), 0).astype(jnp.float32) + 1.0

    def matches(j):
        if j == 0:
            drain(mgot.at[pl.ds(0, inner - 1)], mrecv)
            mgot[seat] = mout[seat]
        weights = []
        for s in range(inner):
            block = mgot[across(s // 2 * 2) - core + s % 2, 2 * j : 2 * j + 2]
            hit[:, s * LANES : (s + 1) * LANES] = (cluster == block[0:1, :]).astype(jnp.bfloat16)
            weight = jnp.where(line == 0, 1.0, 0.0)
            for n, piece in enumerate(pieces(block[1:2, :], 3)):
                weight = jnp.where(line == n + 1, piece.astype(jnp.float32), weight)
            weights.append(jnp.where(lane < cap, weight, 0.0).astype(jnp.bfloat16))
        aux = lax.dot_general(
            jnp.concatenate(weights, axis=1), hit[...], (((1,), (1,)), ((), ())),
            preferred_element_type=jnp.float32,
        )
        if j < last:
            zaux[j] = aux
            aux_copy(j).start()
        else:
            aux_all[...] = aux

    def sources(t, h):
        own = hold.at[t, h, x, y]
        first = xin.at[t, h, y if h == 0 else x]
        direct, passed = yin.at[t, h, 0], yin.at[t, h, 1]
        return (own, first, direct, passed) if h == 0 else (own, direct, first, passed)

    def product(t, h, begin, end):
        stack = []
        for ref in sources(t, h)[begin:end]:
            for s in range(2):
                stack.extend(pieces(ref[s], rep))
        return jnp.dot(
            hit[:, begin * 2 * LANES : end * 2 * LANES], jnp.concatenate(stack, axis=0),
            preferred_element_type=jnp.float32,
        )

    def reduce(j, c):
        t = j * chunks + c
        drain(yin.at[t], yrecv.at[t])
        for h in range(2):
            zout[j, c, :, h * wide : (h + 1) * wide] = product(t, h, 0, 4)

    def conclude(c):
        t = last * chunks + c
        final = t == steps - 1
        if final:
            drain(yin.at[t, :, 0], yrecv.at[steps])
        else:
            drain(yin.at[t], yrecv.at[t])
        for h in range(2):
            total[c, :, h * wide : (h + 1) * wide] = product(t, h, 0, 3 if final else 4)

        @pl.when(plane > 0)
        def _():
            line_arrival(plane, c).wait_recv()
            total[c] += zin[plane, c]

        @pl.when(plane < last)
        def _():
            line_arrival(outer, c).wait_recv()
            total[c] += zin[outer, c]

        if final:
            drain(yin.at[t, :, 1], yrecv.at[t])
        for h in range(2):
            begin = (c + shift) * chunk + h * wide
            value = total[c, :, h * wide : (h + 1) * wide]
            if final:
                value = value + product(t, h, 3, 4)
            if alone:
                square = value * value
                if c == 0 and h == 0:
                    lengths[...] = square
                else:
                    lengths[...] += square
                value = value * inverse[...]
            main_ref[:, begin : begin + wide] = value

    def forward(j, c):
        @pl.when(fed(j))
        def _():
            line_arrival(target_plane(j), c).wait_recv()
            zout[j, c] += zin[target_plane(j), c]
            line_copy(j, c).start()

    def collect():
        if last:
            drain(zin_aux.at[pl.ds(0, last)], arecv)
        for j in range(last):
            aux_all[...] += zin_aux[target_plane(j)]
        if alone:
            denom = jnp.maximum(aux_all[0:1, :], 1.0)
            inverse[...] = 1.0 / jnp.broadcast_to(denom, (LANES, CL_OWN)).T

    def pair_copy(src, dst, ssem, rsem):
        return pltpu.make_async_remote_copy(
            src_ref=src,
            dst_ref=dst,
            send_sem=ssem,
            recv_sem=rsem,
            device_id={"dev": (plane + 1 - 2 * lax.rem(plane, 2)) * inner + seat},
            device_id_type=MESH,
        )

    def pair_label():
        return pair_copy(label_hbm, zlabel, lssem, lrsem)

    def pair_rows():
        return pair_copy(points_ref.at[:, pl.ds(0, chunk)], zraw, rssem, rrsem)

    def pair_plane(m):
        return lax.rem(plane + 2, outer) if m == 0 else plane

    def pair_tell(pair_target):
        zfacts[...] = jnp.concatenate(
            [inside_label(zlabel[...]), jnp.zeros((7, rows), jnp.bfloat16)], axis=0
        )
        for m in range(2):
            for zs, (fact, slots) in enumerate(((facts, target), (zfacts, pair_target))):
                told = lax.dot_general(
                    fact[...], picks(pair_plane(m), slots), (((1,), (1,)), ((), ())),
                    preferred_element_type=jnp.float32,
                )
                for side in range(2):
                    for xx in range(2):
                        row = m * 4 + zs * 2 + xx
                        begin = side * half + xx * LANES
                        zmout[side, row : row + 1] = told[0:1, begin : begin + LANES]
        zmgot[core] = zmout[0]
        for d in range(1, 6):
            plane_copy(zmout.at[d % 2], zmgot.at[d // 2 * 2 + core], zmsend, zmrecv, d).start()

    def pair_core(m, zs):
        return plane_copy(
            zcout.at[m, zs], zhold.at[m, :, :, :, zs * 2 + core], xcsend, xcrecv.at[m], 1
        )

    def pair_first(m, h):
        source = zhold.at[m, 0, 1 - x] if h == 0 else zhold.at[m, 1, :, 1 - y]
        return plane_copy(source, zxin.at[m, h], xfsend, xfrecv.at[m], 2 if h == 0 else 4)

    def pair_sums(m, h):
        return plane_copy(
            zsout.at[m, h], zsin.at[m, h], xssend, xsrecv.at[m], 4 if h == 0 else 2
        )

    def pair_line():
        return pltpu.make_async_remote_copy(
            src_ref=zzout,
            dst_ref=zzin,
            send_sem=zzsend,
            recv_sem=zzrecv,
            device_id={"dev": pair_plane(0) * inner + seat},
            device_id_type=MESH,
        )

    def pair_gather(m, pair_target):
        if m == 0:
            pair_rows().wait_recv()
            value = zraw[...]
            top = value.astype(jnp.bfloat16)
            zhigh[...] = top
            zlow[...] = (value - top.astype(jnp.float32)).astype(jnp.bfloat16)
        for zs in range(2):
            pick = picks(pair_plane(m), pair_target if zs else target)
            upper = zhigh[...] if zs else high[:, :chunk]
            lower = zlow[...] if zs else low[:, :chunk]
            block = jnp.dot(pick, upper, preferred_element_type=jnp.float32)
            block = block + jnp.dot(pick, lower, preferred_element_type=jnp.float32)
            for h in range(2):
                part = block[:, h * wide : (h + 1) * wide]
                zhold[m, h, :, :, zs * 2 + core] = part[:half].reshape(2, 2, cap, wide)
                zcout[m, zs, h] = part[half:].reshape(2, 2, cap, wide)
            pair_core(m, zs).start()

    def pair_product(m, h, away):
        xx = 1 - x if away and h == 1 else x
        yy = 1 - y if away and h == 0 else y
        stack = []
        for side, ref in enumerate((zhold.at[m, h, xx, yy], zxin.at[m, h, yy if h == 0 else xx])):
            for s in range(4):
                got = zmgot[(1 + h) * 2 * side + s % 2, pl.ds(m * 4 + s // 2 * 2 + xx, 1)]
                label = jnp.where(
                    yy == 1,
                    jnp.concatenate([got[:, cap:]] * 2, axis=1),
                    jnp.concatenate([got[:, :cap]] * 2, axis=1),
                )
                n = side * 4 + s
                zhit[:, n * LANES : (n + 1) * LANES] = (cluster == label).astype(jnp.bfloat16)
                stack.extend(pieces(ref[s], rep))
        return jnp.dot(
            zhit[...], jnp.concatenate(stack, axis=0), preferred_element_type=jnp.float32
        )

    def pair_send(m):
        if m == 0:
            drain(zmgot.at[pl.ds(0, 5)], zmrecv)
        for h in range(2):
            zsout[m, h] = pair_product(m, h, True)
            pair_sums(m, h).start()

    def pair_arrange(m):
        for h in range(2):
            columns = slice(h * wide, (h + 1) * wide)
            own = zzout if m == 0 else zzown
            own[:, columns] = pair_product(m, h, False)
        drain(zsin.at[m], xsrecv.at[m])
        for h in range(2):
            columns = slice(h * wide, (h + 1) * wide)
            own = zzout if m == 0 else zzown
            own[:, columns] += zsin[m, h]
        if m == 0:
            pair_line().start()

    def pair_conclude():
        pair_line().wait_recv()
        for h in range(2):
            columns = slice(h * wide, (h + 1) * wide)
            value = zzown[:, columns] + zzin[:, columns]
            if alone:
                lengths[...] += value * value
                value = value * inverse[...]
            main_ref[:, columns] = value

    load_label().start()
    load(shift).start()
    barrier = pltpu.get_barrier_semaphore()
    for d in range(1, inner):
        peer = plane * inner + across(d)
        pl.semaphore_signal(barrier, inc=1, device_id={"dev": peer}, device_id_type=MESH)
    for d in range(1, outer):
        peer = lax.rem(plane + d, outer) * inner + seat
        pl.semaphore_signal(barrier, inc=1, device_id={"dev": peer}, device_id_type=MESH)

    load_label().wait()
    target = route(label_ref[...])
    pick = picks(target_plane(0), target)
    split(shift)
    for c in range(width // chunk):
        if c != shift:
            load(c).start()
    gather(0, pick, 0, half)
    pl.semaphore_wait(barrier, inner + outer - 2)
    for h in range(2):
        first_copy(0, h, 0).start()
    if paired:
        pair_label().start()
        pair_rows().start()
    gather(0, pick, half, 2 * half)
    core_copy(0).start()

    def prepare(t):
        nonlocal pick
        if t < chunks:
            split(t + shift)
        if t % chunks == 0:
            pick = picks(target_plane(t // chunks), target)
        gather(t, pick)
        core_copy(t).start()

    def push(t):
        core_arrival(t).wait_recv()
        for h in range(2):
            first_copy(t, h, parts_of(t) - 1).start()

    def pair_push(m):
        drain(zcout.at[m], xcrecv.at[m])
        for h in range(2):
            pair_first(m, h).start()

    def direct(t):
        for h in range(2):
            direct_copy(t, h).start()

    def head(t):
        drain(xin.at[t], frecv.at[t])
        for h in range(2):
            passed_copy(t, h).start()

    def arrange(t):
        j, c = t // chunks, t % chunks
        if c == 0:
            matches(j)
        if j == last:
            if c == 0:
                collect()
            conclude(c)
            return
        reduce(j, c)

        @pl.when(jnp.logical_not(fed(j)))
        def _():
            line_copy(j, c).start()

    split(1 + shift)
    gather(1, pick, 0, half)
    for h in range(2):
        first_copy(1, h, 0).start()
    gather(1, pick, half, 2 * half)
    core_copy(1).start()
    push(0)
    direct(0)
    prepare(2)
    push(1)
    if paired:
        split(0)
    tell()
    for j in range(outer - 1):
        tell_slots(j, picks(target_plane(j), target))
    head(0)
    tell_slots(last, picks(target_plane(last), target))
    for d in range(1, inner):
        meta_copy(d).start()
    push(2)
    direct(1)
    prepare(3)

    if paired:
        head(1)
        push(3)
        direct(2)
        pair_label().wait_recv()
        pair_target = route(zlabel[...])
        pair_tell(pair_target)
        prepare(4)
        arrange(0)

        head(2)
        push(4)
        direct(3)
        prepare(5)
        arrange(1)

        head(3)
        push(5)
        direct(4)
        arrange(2)
        pair_gather(0, pair_target)

        head(4)
        pair_push(0)
        direct(5)
        forward(0, 0)
        prepare(6)
        arrange(3)

        head(5)
        pair_gather(1, pair_target)
        arrange(4)
        forward(0, 1)
        pair_push(1)

        drain(zxin.at[0], xfrecv.at[0])
        pair_send(0)
        push(6)
        prepare(7)
        forward(2, 0)
        forward(1, 0)
        arrange(5)
        forward(2, 1)
        forward(1, 1)

        drain(zxin.at[1], xfrecv.at[1])
        pair_send(1)
        push(7)
        direct(6)
        pair_arrange(0)

        head(6)
        direct(7)
        pair_arrange(1)

        head(7)
        arrange(6)
        arrange(7)
        pair_conclude()
    else:
        waiting = []
        for t in range(1, steps + 1):
            if t < steps:
                head(t)
            if t + 2 < steps:
                push(t + 2)
            if t + 1 < steps:
                direct(t + 1)
            if t + 3 < steps:
                prepare(t + 3)
            arrange(t - 1)
            j, c = (t - 1) // chunks, (t - 1) % chunks
            if j == last - 1:
                forward(j, c)
            elif j < last:
                waiting.append((j, c))
            while waiting and (len(waiting) > 2 or t >= last * chunks):
                forward(*waiting.pop(0))
    if alone:
        denom = jnp.maximum(aux_all[0:1, :], 1.0)
        squares = aux_all[1:2, :] + aux_all[2:3, :] + aux_all[3:4, :]
        length = jnp.sum(lengths[...].T, axis=0, keepdims=True)
        side_ref[...] = (squares - length / denom) / (denom * width)
    else:
        side_ref[...] = aux_all[...]

    drain(mout.at[pl.ds(0, inner - 1)], msend)
    for t in range(max(steps - ring, 0), steps):
        core_copy(t).wait_send()
    drain(xin, fsend)
    drain(yin, ysend)
    if last:
        drain(zout, zsend)
        drain(zaux, asend)
    if paired:
        pair_label().wait_send()
        pair_rows().wait_send()
        drain(zmgot.at[pl.ds(0, 5)], zmsend)
        drain(zcout, xcsend)
        drain(zxin, xfsend)
        drain(zsout, xssend)
        pair_line().wait_send()


def body(points, assignment):
    owners = lax.axis_size("dev")
    alone = lax.axis_size("grp") == 1
    rows, width = points.shape
    cap = 2 * rows // owners
    outer = owners // INNER
    chunk = 2 * LANES
    paired = outer == 4 and 2 * cap == LANES and width == 3 * chunk
    chunks = width // chunk - (1 if paired else 0)
    wide = chunk // 2
    steps = outer * chunks
    ring = min(steps, 4)

    f32, b16 = jnp.float32, jnp.bfloat16
    dma = pltpu.SemaphoreType.DMA
    hops = max(outer - 1, 1)
    side = (1, CL_OWN) if alone else (8, CL_OWN)
    extra = [
        pltpu.VMEM((1, rows), jnp.int32),
        pltpu.VMEM((rows, chunk), f32),
        pltpu.VMEM((rows, chunk), b16),
        pltpu.VMEM((rows, chunk), b16),
        pltpu.VMEM((8, rows), b16),
        pltpu.VMEM((2, 2, 2, 2, 4, cap, wide), f32),
        pltpu.VMEM((2, 2, 2, 2, 2, cap, wide), f32),
        pltpu.VMEM((2, 2, 2, 4, cap, wide), f32),
        pltpu.VMEM((2, 2, CL_OWN, wide), f32),
        pltpu.VMEM((2, 2, CL_OWN, wide), f32),
        pltpu.VMEM((CL_OWN, chunk), f32),
        pltpu.VMEM((CL_OWN, chunk), f32),
        pltpu.VMEM((CL_OWN, chunk), f32),
        pltpu.VMEM((2, 8, LANES), f32),
        pltpu.VMEM((6, 8, LANES), f32),
        pltpu.VMEM((CL_OWN, INNER * LANES), b16),
        dma(()), dma(()), dma(()), dma(()),
        dma(()), dma((2,)), dma(()), dma((2,)),
        dma(()), dma((2,)), dma(()), dma(()), dma(()), dma(()),
    ]
    vmem = pl.BlockSpec(memory_space=pltpu.VMEM)
    hbm = pl.BlockSpec(memory_space=pltpu.HBM)
    main, side = pl.pallas_call(
        functools.partial(kernel, outer, cap, chunk, alone, paired),
        out_shape=(
            jax.ShapeDtypeStruct((CL_OWN, width), f32),
            jax.ShapeDtypeStruct(side, f32),
        ),
        in_specs=[hbm, hbm],
        out_specs=[vmem, vmem],
        scratch_shapes=[
            pltpu.VMEM((1, rows), jnp.int32),
            pltpu.VMEM((width // chunk, rows, chunk), f32),
            pltpu.VMEM((rows, width), b16),
            pltpu.VMEM((rows, width), b16),
            pltpu.VMEM((rows, LANES), f32),
            pltpu.VMEM((8, rows), b16),
            pltpu.VMEM((CL_OWN, INNER * LANES), b16),
            pltpu.VMEM((steps, 2, 2, 2, 2, cap, wide), f32),
            pltpu.VMEM((ring, 2, 2, 2, cap, wide), f32),
            pltpu.VMEM((steps, 2, 2, 2, cap, wide), f32),
            pltpu.VMEM((steps, 2, 2, 2, cap, wide), f32),
            pltpu.VMEM((INNER, 2 * outer, LANES), f32),
            pltpu.VMEM((INNER, 2 * outer, LANES), f32),
            pltpu.VMEM((hops, chunks, CL_OWN, chunk), f32),
            pltpu.VMEM((outer + 1, chunks, CL_OWN, chunk), f32),
            pltpu.VMEM((hops, 8, CL_OWN), f32),
            pltpu.VMEM((outer, 8, CL_OWN), f32),
            pltpu.VMEM((chunks, CL_OWN, chunk), f32),
            pltpu.VMEM((8, CL_OWN), f32),
            pltpu.VMEM((CL_OWN, LANES), f32),
            pltpu.VMEM((CL_OWN, LANES), f32),
            dma((width // chunk + 1,)),
            dma(()), dma(()),
            dma((ring,)), dma((steps,)),
            dma(()), dma((steps,)),
            dma(()), dma((steps + 1,)),
            dma(()), dma((outer + 1, chunks)),
            dma(()), dma(()),
        ] + (extra if paired else []),
        compiler_params=pltpu.CompilerParams(
            collective_id=0, has_side_effects=True, vmem_limit_bytes=LIMIT
        ),
    )(points, pltpu.with_memory_space_constraint(assignment.reshape(1, rows), pltpu.HBM))
    if alone:
        return main, side[0]
    squares = side[1] + side[2] + side[3]
    sums, counts, squares = lax.psum((main, side[0], squares), "grp")
    return finish(sums, counts, squares)


def solution(mesh):
    return jax.shard_map(
        body,
        mesh=mesh,
        in_specs=(P(("grp", "dev"), None), P(("grp", "dev"))),
        out_specs=(P("dev", None), P("dev")),
        check_vma=False,
    )
```
